32 devices in a mesh: dp: 4 (over y, core), expert: 4 (over z), pipe: 2 (over x).
Axes of the slice: x: 2, y: 2, z: 4, core: 2. Of those that a mesh axis runs over, the one named last changes fastest.
Arguments:
- inputs: bfloat16 [512, 4096], P('expert'), may hold values from -6 to 6
- cotangents: bfloat16 [512, 4096], P('expert'), may hold values from -6 to 6
- routes: int32 [512, 2], P('expert'), may hold values from 0 to 3, all different within a row; in each aligned block of 128 rows (0 to 127, 128 to 255, ...) at most 128 rows name the same one
- gates: float32 [512, 2], P('expert'), may hold values from 0.1 to 1
- w_gate: bfloat16 [4, 4096, 7168], P('expert', None, ('dp', 'pipe')), may hold values from -0.09375 to 0.09375
- w_up: bfloat16 [4, 4096, 7168], P('expert', None, ('dp', 'pipe')), may hold values from -0.09375 to 0.09375
- w_down: bfloat16 [4, 7168, 4096], P('expert', ('dp', 'pipe')), may hold values from -0.09375 to 0.09375
- proj_in: bfloat16 [4096, 32], replicated, may hold values from -0.09375 to 0.09375
- proj_out: bfloat16 [4096, 64], replicated, may hold values from -0.09375 to 0.09375
- proj_hid_a: bfloat16 [7168, 32], P(('dp', 'pipe')), may hold values from -0.0625 to 0.0625
- proj_hid_b: bfloat16 [7168, 64], P(('dp', 'pipe')), may hold values from -0.0625 to 0.0625
- queries: bfloat16 [256, 6144], P(('dp', 'pipe')), may hold values from -0.078125 to 0.078125
Outputs:
- token_scores: float32 [512, 256], P('expert', ('dp', 'pipe'))
- query_totals: float32 [256], P(('dp', 'pipe'))
The draws below stay inside these ranges and needn't reach their ends.
Inputs may be any that keep to these rules, and one draw needn't show every extreme that they name: `routes`: each row names two different experts. Among the 128 tokens of one index of expert (aligned blocks), no expert is named more than 128 times, and in some blocks one expert is named exactly 128 times.
All inputs are finite; a program needn't handle non-finite values.
Results may differ from the reference program's by a relative error of at most 0.0041.
Values may be sent and summed in bfloat16 or wider, within the bound.
A program may use at most 128 MiB of HBM per device.

```python
import math
import jax
import jax.numpy as jnp
import numpy as np
from jax import lax

D = 4096
FF = 7168
KA = 32
KB = 64
NQ = 256
TOK_DEV = 128
EXPERTS = 4
TOKENS = 512
CAP = 128
SKETCH = 6144
N_EXPERT = 4


def block_levels(stream_key, extent, pieces, low, top_value):
    def one(dim, shards_of):
        steps = jax.random.uniform(jax.random.fold_in(jax.random.fold_in(stream_key, 6), dim), (shards_of,), jnp.float32, low / len(pieces), top_value / len(pieces))
        return jnp.repeat(jnp.exp(steps), extent[dim] // shards_of).reshape((-1,) + (1,) * (len(extent) - dim - 1))

    gain = one(*pieces[0])
    for cut in pieces[1:]:
        gain = gain * one(*cut)
    return gain


def shared_out(stream_key, own, number, rows, count, top, bound, skew):
    order = jax.random.permutation(stream_key, count)
    crowded, common = portions_of(count, rows * top, bound, skew, True), portions_of(count, rows * top, bound, skew, False)
    places = jnp.arange(count)

    def named(sizes, rotation):
        used = int((sizes > 0).sum())
        fixed = max(1, used // 4)
        passed = fixed + (places - fixed + rotation * (used - fixed)) % max(1, count - fixed)
        return jnp.zeros((count,), jnp.int32).at[order[jnp.where(places < fixed, places, passed)]].set(jnp.asarray(sizes, jnp.int32))

    sizes = jnp.where(number % 4 == 0, named(crowded, number // 4), named(common, number - number // 4 - 1))
    mixed = jax.random.permutation(jax.random.fold_in(own, 3), count)
    source_of, taker = mixed[0:count // 2 * 2:2], mixed[1:count // 2 * 2:2]
    room = jnp.minimum(sizes[source_of] - 1, bound - sizes[taker]) // 2
    room = jnp.where((source_of == order[0]) | (taker == order[0]) | (sizes[taker] == 0), 0, jnp.maximum(room, 0))
    passed = jax.random.randint(jax.random.fold_in(own, 4), (count // 2,), 0, 1 << 20) % (room + 1)
    sizes = sizes.at[source_of].add(-passed).at[taker].add(passed)
    items = jnp.searchsorted(jnp.cumsum(sizes), jnp.arange(rows * top), side="right").astype(jnp.int32)
    table = items.reshape(top, rows).T
    table = table[jax.random.permutation(jax.random.fold_in(own, 1), rows)]
    rotation = jax.random.randint(jax.random.fold_in(own, 2), (rows, 1), 0, top)
    return jnp.take_along_axis(table, (jnp.arange(top)[None, :] + rotation) % top, axis=1)


def portions_of(count, total, bound, slope, full):
    loads = [(1 << 20) // math.isqrt(rank ** slope) + 1 for rank in range(1, count + 1)]
    largest = bound if full else min(bound, max(-(-total // count), total * loads[0] // sum(loads)))
    least = 1 if total - largest >= count - 1 else 0
    given, surplus = [largest] + [least] * (count - 1), total - largest - least * (count - 1)
    while surplus > 0:
        candidates = [i for i in range(1, count) if given[i] < largest] or [i for i in range(1, count) if given[i] < bound]
        pool, left = sum([loads[i] for i in candidates]), surplus
        for i in candidates:
            more = min(bound - given[i], max(1, left * loads[i] // pool), surplus)
            given[i] = given[i] + more
            surplus = surplus - more
    return np.array(given)


def scatter_about(rng, dims, deviation, most, shards=(), kind=jnp.bfloat16):
    drawn = deviation * jax.random.normal(rng, dims, jnp.float32)
    if shards:
        drawn = drawn * block_levels(rng, dims, shards, -0.22, 0.18)
    return jnp.clip(drawn, -most, most).astype(kind)


def setup_inputs(seed: int = 0) -> dict:
    splits = jax.random.split(jax.random.key(seed), 13)
    inputs = scatter_about(splits[0], (TOKENS, D), 1.0, 6.0, ((0, 4),))
    cotangents = scatter_about(splits[1], (TOKENS, D), 1.0, 6.0, ((0, 4),))
    routes_keys = jax.random.split(jax.random.fold_in(splits[2], 1), TOKENS // TOK_DEV)
    routes_turns = jax.random.permutation(jax.random.fold_in(splits[2], 3), TOKENS // TOK_DEV)
    routes = jax.vmap(lambda own, number: shared_out(jax.random.fold_in(splits[2], 2), own, number, TOK_DEV, EXPERTS, 2, CAP, 2))(routes_keys, routes_turns).reshape((TOKENS, 2))
    gates = jnp.clip(jnp.exp(math.log(1.0) - 2.3025851 * jax.random.uniform(splits[3], (TOKENS, 2), jnp.float32) ** block_levels(splits[3], (TOKENS, 2), ((0, 4),), -0.2, 0.2)), 0.1, 1.0)
    w_gate = scatter_about(splits[4], (EXPERTS, D, FF), D ** -0.5, 0.09375, ((0, 4), (2, 8)))
    w_up = scatter_about(splits[5], (EXPERTS, D, FF), D ** -0.5, 0.09375, ((0, 4), (2, 8)))
    w_down = scatter_about(splits[6], (EXPERTS, FF, D), D ** -0.5, 0.09375, ((0, 4), (1, 8)))
    proj_in = scatter_about(splits[7], (D, KA), D ** -0.5, 0.09375)
    proj_out = scatter_about(splits[8], (D, KB), D ** -0.5, 0.09375)
    proj_hid_a = scatter_about(splits[9], (FF, KA), FF ** -0.5, 0.0625, ((0, 8),))
    proj_hid_b = scatter_about(splits[10], (FF, KB), FF ** -0.5, 0.0625, ((0, 8),))
    queries = scatter_about(splits[11], (NQ, SKETCH), SKETCH ** -0.5, 0.078125, ((0, 8),))
    return dict(inputs=inputs, cotangents=cotangents, routes=routes, gates=gates, w_gate=w_gate, w_up=w_up, w_down=w_down, proj_in=proj_in, proj_out=proj_out, proj_hid_a=proj_hid_a, proj_hid_b=proj_hid_b, queries=queries)


def slot_matrix(route_rows, gate_rows, experts, capacity):
    count = route_rows.shape[0]
    flat = route_rows.reshape(-1)
    labels = jnp.arange(experts, dtype=jnp.int32)
    onehot = (flat[:, None] == labels[None, :]).astype(jnp.int32)
    earlier = jnp.cumsum(onehot, axis=0) - onehot
    position = lax.optimization_barrier(jnp.sum(onehot * (labels[None, :] * capacity + earlier), axis=1))
    slot_ids = jnp.arange(experts * capacity, dtype=jnp.int32)
    table = (position[None, :] == slot_ids[:, None]).astype(jnp.float32).reshape(experts * capacity, count, 2)
    picks = lax.optimization_barrier(jnp.sum(table, axis=2))
    weighted = lax.optimization_barrier(jnp.sum(table * gate_rows[None, :, :], axis=2))
    return (picks, weighted)

def expert_scores(rows_in, rows_back, gate_proj, up_proj, down_proj, input_proj, output_proj, hidden_proj, grad_proj, query_rows):
    gate_pre = jnp.dot(rows_in, gate_proj, preferred_element_type=jnp.float32)
    up_pre = jnp.dot(rows_in, up_proj, preferred_element_type=jnp.float32)
    sigma = jax.nn.sigmoid(gate_pre)
    hidden = (gate_pre * sigma * up_pre).astype(jnp.bfloat16)
    a_input = jnp.dot(rows_in, input_proj, preferred_element_type=jnp.float32)
    a_hidden = jnp.dot(hidden, hidden_proj, preferred_element_type=jnp.float32)
    back = lax.dot_general(rows_back, down_proj, (((1,), (1,)), ((), ())), preferred_element_type=jnp.float32)
    d_up = (back * gate_pre * sigma).astype(jnp.bfloat16)
    d_gate = (back * up_pre * sigma * (1.0 + gate_pre * (1.0 - sigma))).astype(jnp.bfloat16)
    b_output = jnp.dot(rows_back, output_proj, preferred_element_type=jnp.float32)
    b_up = jnp.dot(d_up, grad_proj, preferred_element_type=jnp.float32)
    b_gate = jnp.dot(d_gate, grad_proj, preferred_element_type=jnp.float32)
    height = rows_back.shape[0]
    sketch = jnp.concatenate([(a_hidden[:, :, None] * b_output[:, None, :]).reshape(height, -1), (a_input[:, :, None] * b_up[:, None, :]).reshape(height, -1), (a_input[:, :, None] * b_gate[:, None, :]).reshape(height, -1)], axis=1).astype(jnp.bfloat16)
    return lax.dot_general(sketch, query_rows, (((1,), (1,)), ((), ())), preferred_element_type=jnp.float32)

def reference(inputs, cotangents, routes, gates, w_gate, w_up, w_down, proj_in, proj_out, proj_hid_a, proj_hid_b, queries):
    sources = N_EXPERT
    rows_in = inputs.reshape(sources, TOK_DEV, D)
    rows_back = cotangents.reshape(sources, TOK_DEV, D)
    picks, weighted = jax.vmap(lambda r, g: slot_matrix(r, g, EXPERTS, CAP))(routes.reshape(sources, TOK_DEV, 2), gates.reshape(sources, TOK_DEV, 2))

    def dispatch(index):
        pick = picks[index].astype(jnp.bfloat16)
        first = jnp.dot(pick, rows_in[index], preferred_element_type=jnp.float32).astype(jnp.bfloat16)
        second = jnp.dot(pick, rows_back[index], preferred_element_type=jnp.float32).astype(jnp.bfloat16)
        return (first, second)
    slots_in, slots_back = lax.map(dispatch, jnp.arange(sources, dtype=jnp.int32))
    slots_in = slots_in.reshape(sources, EXPERTS, CAP, D).transpose(1, 0, 2, 3).reshape(EXPERTS, sources * CAP, D)
    slots_back = slots_back.reshape(sources, EXPERTS, CAP, D).transpose(1, 0, 2, 3).reshape(EXPERTS, sources * CAP, D)

    def per_expert(expert):
        return expert_scores(slots_in[expert], slots_back[expert], w_gate[expert], w_up[expert], w_down[expert], proj_in, proj_out, proj_hid_a, proj_hid_b, queries)
    scores = lax.map(per_expert, jnp.arange(EXPERTS, dtype=jnp.int32))
    scores = scores.reshape(EXPERTS, sources, CAP, NQ).transpose(1, 0, 2, 3).reshape(sources, EXPERTS * CAP, NQ)

    def combine(index):
        return lax.dot_general(weighted[index], scores[index], (((0,), (0,)), ((), ())), precision=lax.Precision.HIGHEST, preferred_element_type=jnp.float32)
    token_scores = lax.map(combine, jnp.arange(sources, dtype=jnp.int32)).reshape(TOKENS, NQ)
    query_totals = lax.optimization_barrier(jnp.sum(token_scores, axis=0)) * (1.0 / math.sqrt(TOKENS))
    return (token_scores, query_totals)
```

```python
import functools
import math

import jax
import jax.numpy as jnp
from jax import lax
from jax.experimental import pallas as pl
from jax.experimental.pallas import tpu as pltpu
from jax.sharding import PartitionSpec as P

MESH = pl.DeviceIdType.MESH
F32 = jnp.float32
BF16 = jnp.bfloat16
NT = (((1,), (1,)), ((), ()))


def slot_matrix(route_rows, gate_rows, experts, capacity):
    count = route_rows.shape[0]
    flat = route_rows.reshape(-1)
    labels = jnp.arange(experts, dtype=jnp.int32)
    onehot = (flat[:, None] == labels[None, :]).astype(jnp.int32)
    earlier = jnp.cumsum(onehot, axis=0) - onehot
    position = jnp.sum(onehot * (labels[None, :] * capacity + earlier), axis=1)
    slot_ids = jnp.arange(experts * capacity, dtype=jnp.int32)
    table = (
        (position[None, :] == slot_ids[:, None]).astype(F32).reshape(experts * capacity, count, 2)
    )
    picks = jnp.sum(table, axis=2)
    weighted = jnp.sum(table * gate_rows[None, :, :], axis=(1, 2))
    return (picks, weighted)


def mega(
    dims,
    buf_in,
    buf_back,
    weight_own,
    wg_hbm,
    wu_hbm,
    wd_hbm,
    p_in,
    p_out,
    p_a,
    p_b,
    query,
    ret_ref,
    tot_ref,
    x_in,
    x_back,
    wg,
    wu,
    wd,
    gate_s,
    up_s,
    ain_s,
    bout_s,
    part,
    land,
    red,
    wl,
    sc,
    ret,
    tsrc,
    tland,
    local_sem,
    z_send,
    z_recv,
    y_send,
    y_recv,
    x_send,
    x_recv,
    g1_send,
    g1_recv,
    g2_send,
    g2_recv,
    c_send,
    c_recv,
    w_send,
    w_recv,
    rs_send,
    rs_recv,
    ag_send,
    ag_recv,
    e_send,
    e_recv,
    t_send,
    t_recv,
):
    E, DP, NP, L, cap, ka, kb = dims
    H = DP // L
    N = DP * NP
    R = E * cap
    width = x_in.shape[1]
    cw = width // N
    hw = cw // 2
    G = 128 // ka
    rk = R // G
    dp = lax.axis_index("dp")
    me = lax.axis_index("expert")
    p = lax.axis_index("pipe")
    h = dp // L
    l = dp % L
    s = dp * NP + p

    def dev(d, e, q):
        return {"dp": d, "expert": e, "pipe": q}

    locals_ = []
    dense = buf_in.shape[0] == 1
    own = 0 if dense else me
    for i, (src, dst) in enumerate(
        (
            (buf_in.at[own], x_in.at[pl.ds(0, cap), :]),
            (buf_back.at[own], x_back.at[pl.ds(0, cap), :]),
            (weight_own.at[me], wl.at[pl.ds(0, cap), :]),
            (wg_hbm.at[0], wg),
            (wu_hbm.at[0], wu),
            (wd_hbm.at[0], wd),
        )
    ):
        c = pltpu.make_async_copy(src, dst, local_sem.at[i])
        locals_.append(c)

    barrier = pltpu.get_barrier_semaphore()

    def plane(k):
        t = lax.rem(s + k, N)
        return dev(t // NP, me, t % NP)

    for k in range(1, N):
        pl.semaphore_signal(barrier, inc=1, device_id=plane(k), device_id_type=MESH)
    for k in range(1, E):
        pl.semaphore_signal(
            barrier, inc=1, device_id=dev(dp, lax.rem(me + k, E), p), device_id_type=MESH
        )
    pl.semaphore_wait(barrier, N + E - 2)

    bufs = (buf_in, buf_back)
    xs = (x_in, x_back)

    def rc(src, dst, ss, rs, to):
        return pltpu.make_async_remote_copy(
            src_ref=src, dst_ref=dst, send_sem=ss, recv_sem=rs, device_id=to, device_id_type=MESH
        )

    def cols(share, off=0, size=None):
        size = cw if size is None else size
        return pl.ds(pl.multiple_of(share * cw + off, 128), size)

    def rows(d):
        return pl.ds(pl.multiple_of(d * cap, 8), cap)

    def share(k, kp, lane=None):
        lane = l if lane is None else lane
        return (lax.rem(h - k + H, H) * L + lane) * NP + lax.rem(p - kp + NP, NP)

    def zc(a, d):
        dst = lax.rem(me - d + E, E)
        src = bufs[a].at[0 if dense else dst, :, cols(s)]
        return rc(src, xs[a].at[rows(d), cols(s)], z_send.at[a, d - 1], z_recv.at[a, d - 1], dev(dp, dst, p))

    def yc(a, k, d):
        r = xs[a].at[rows(d), cols(s)]
        return rc(r, r, y_send.at[a, k - 1, d - 1], y_recv.at[a, k - 1, d - 1], dev(lax.rem(h + k, H) * L + l, me, p))

    def xc(a, kp, d):
        r = xs[a].at[rows(d), cols(s)]
        return rc(r, r, x_send.at[a, kp - 1, d - 1], x_recv.at[a, kp - 1, d - 1], dev(dp, me, lax.rem(p + kp, NP)))

    def g1(a, k, kp, d):
        r = xs[a].at[rows(d), cols(share(k, 0), 0, hw)]
        i = (a, k - 1, kp - 1, d - 1)
        return rc(r, r, g1_send.at[i], g1_recv.at[i], dev(dp, me, lax.rem(p + kp, NP)))

    def g2(a, k, kp, d):
        r = xs[a].at[rows(d), cols(share(0, kp), hw, hw)]
        i = (a, k - 1, kp - 1, d - 1)
        return rc(r, r, g2_send.at[i], g2_recv.at[i], dev(lax.rem(h + k, H) * L + l, me, p))

    def cc(a, k, kp, d):
        r = xs[a].at[rows(d), cols(share(k, kp))]
        i = (a, k, kp, d - 1)
        return rc(r, r, c_send.at[i], c_recv.at[i], dev(h * L + (1 - l), me, p))

    def wc(d):
        dst = lax.rem(me - d + E, E)
        return rc(weight_own.at[dst], wl.at[rows(d), :], w_send.at[d - 1], w_recv.at[d - 1], dev(dp, dst, p))

    def each(fn):
        def step(i, carry):
            fn(i + 1)
            return carry

        lax.fori_loop(0, E - 1, step, 0)

    KS = range(1, H)
    PS = range(1, NP)

    def stage_a(a):
        def f(d):
            zc(a, d).wait_recv()
            for k in KS:
                yc(a, k, d).start()
            for kp in PS:
                xc(a, kp, d).start()
            if L > 1:
                cc(a, 0, 0, d).start()

        each(f)

    def stage_b(a):
        def f(d):
            for k in KS:
                yc(a, k, d).wait_recv()
                for kp in PS:
                    g1(a, k, kp, d).start()
                if L > 1:
                    cc(a, k, 0, d).start()
            for kp in PS:
                xc(a, kp, d).wait_recv()
                for k in KS:
                    g2(a, k, kp, d).start()
                if L > 1:
                    cc(a, 0, kp, d).start()

        each(f)

    def stage_c(a):
        def f(d):
            for k in KS:
                for kp in PS:
                    g1(a, k, kp, d).wait_recv()
                    g2(a, k, kp, d).wait_recv()
                    if L > 1:
                        cc(a, k, kp, d).start()

        each(f)

    def stage_d(a):
        def f(d):
            if L > 1:
                for k in range(H):
                    for kp in range(NP):
                        cc(a, k, kp, d).wait_recv()

        each(f)

    def drain(a):
        def f(d):
            zc(a, d).wait_send()
            for k in KS:
                yc(a, k, d).wait_send()
            for kp in PS:
                xc(a, kp, d).wait_send()
            for k in KS:
                for kp in PS:
                    g1(a, k, kp, d).wait_send()
                    g2(a, k, kp, d).wait_send()
            if L > 1:
                for k in range(H):
                    for kp in range(NP):
                        cc(a, k, kp, d).wait_send()

        each(f)

    each(lambda d: zc(0, d).start())
    each(lambda d: zc(1, d).start())
    for c in locals_:
        c.start()
    each(lambda d: wc(d).start())
    stage_a(0)
    stage_b(0)
    stage_a(1)
    stage_c(0)
    stage_d(0)
    for i in (0, 3, 4):
        locals_[i].wait()

    MT = min(256, R)
    T = R // MT
    lane = lax.broadcasted_iota(jnp.int32, (MT, 128), 1)
    part[pl.ds(R, rk), :] = jnp.zeros((rk, 128), F32)

    def gate_up(m):
        rr = pl.ds(pl.multiple_of(m * MT, MT), MT)
        x = x_in[rr, :]
        g = jnp.dot(x, wg[...], preferred_element_type=F32)
        gate_s[rr, :] = g
        u = jnp.dot(x, wu[...], preferred_element_type=F32)
        up_s[rr, :] = u
        ain_s[rr, :] = jnp.dot(x, p_in[...], preferred_element_type=F32)

    def factor_a(m):
        rr = pl.ds(pl.multiple_of(m * MT, MT), MT)
        g = gate_s[rr, :]
        u = up_s[rr, :]
        sg = jax.nn.sigmoid(g)
        gs = g * sg
        hid = (gs * u).astype(BF16)
        gate_s[rr, :] = gs
        up_s[rr, :] = u * sg * (1.0 + g * (1.0 - sg))
        at = jnp.dot(hid, p_a[...], preferred_element_type=F32)
        for j in range(MT // rk):
            grp = m * (MT // rk) + j
            piece = at[j * rk : (j + 1) * rk, :]
            part[pl.ds(R, rk), :] += jnp.where(lane[:rk] // ka == grp, piece, 0.0)

    def down(m):
        rr = pl.ds(pl.multiple_of(m * MT, MT), MT)
        x = x_back[rr, :]
        back = lax.dot_general(x, wd[...], NT, preferred_element_type=F32)
        bout_s[rr, :] = jnp.dot(x, p_out[...], preferred_element_type=F32)
        du = (back * gate_s[rr, :]).astype(BF16)
        dg = (back * up_s[rr, :]).astype(BF16)
        bu = jnp.dot(du, p_b[...], preferred_element_type=F32)
        bg = jnp.dot(dg, p_b[...], preferred_element_type=F32)
        part[rr, :] = jnp.where(lane < kb, bu, bg)

    half = (T + 1) // 2
    pl.loop(0, half)(gate_up)
    stage_b(1)
    if T > half:
        pl.loop(half, T)(gate_up)
    stage_c(1)
    pl.loop(0, T)(factor_a)
    stage_d(1)
    locals_[1].wait()
    locals_[5].wait()
    pl.loop(0, T)(down)

    ch = (R + rk) // N

    def chunk(i):
        return pl.ds(pl.multiple_of(i * ch, 8), ch)

    def rsc(k):
        t = lax.rem(s + k, N)
        return rc(part.at[chunk(t), :], land.at[k - 1], rs_send.at[k - 1], rs_recv.at[k - 1], plane(k))

    def agc(k):
        r = red.at[chunk(s), :]
        return rc(r, r, ag_send.at[k - 1], ag_recv.at[k - 1], plane(k))

    for k in range(1, N):
        rsc(k).start()
    for k in range(1, N):
        rsc(k).wait_recv()
    total = part[chunk(s), :]
    for k in range(1, N):
        total = total + land[k - 1]
    red[chunk(s), :] = total
    for k in range(1, N):
        agc(k).start()
    each(lambda d: wc(d).wait_recv())
    locals_[2].wait()
    for k in range(1, N):
        t = lax.rem(s - k + N, N)
        r = red.at[chunk(t), :]
        rc(r, r, ag_send.at[k - 1], ag_recv.at[k - 1], plane(k)).wait_recv()

    seg = ka * kb
    lane_k = lax.broadcasted_iota(jnp.int32, (rk, 128), 1)

    def split(a):
        hi = a.astype(BF16)
        return hi, (a - hi.astype(F32)).astype(BF16)

    def spread(a, first):
        depth = a.shape[1]
        row = lax.broadcasted_iota(jnp.int32, (depth, seg), 0)
        col = lax.broadcasted_iota(jnp.int32, (depth, seg), 1)
        sel = jnp.where(row - first == col // kb, 1.0, 0.0).astype(BF16)
        hi, lo = split(a)
        return jnp.dot(hi, sel, preferred_element_type=F32) + jnp.dot(
            lo, sel, preferred_element_type=F32
        )

    def score(k):
        rr = pl.ds(pl.multiple_of(k * rk, 8), rk)
        b = red[rr, :]
        br = pltpu.roll(b, kb, 1)
        bu = jnp.where(lane_k < kb, b, br)
        bg = jnp.where(lane_k < kb, br, b)
        ah = spread(red[pl.ds(R, rk), :], k * ka)
        ai = spread(ain_s[rr, :], 0)
        q = query[...]
        reps = seg // 128

        def seg_dot(a, bb, i):
            sk = jnp.concatenate(
                [(a[:, j * 128 : (j + 1) * 128] * bb).astype(BF16) for j in range(reps)], axis=1
            )
            return lax.dot_general(
                sk, q[:, i * seg : (i + 1) * seg], NT, preferred_element_type=F32
            )

        r = seg_dot(ah, bout_s[rr, :], 0) + seg_dot(ai, bu, 1) + seg_dot(ai, bg, 2)
        sc[rr, :] = r * wl[rr, :]

    pl.loop(0, G)(score)
    tsrc[...] = jnp.broadcast_to(jnp.sum(sc[...], axis=0, keepdims=True), tsrc.shape)

    def ec(d):
        return rc(sc.at[rows(d), :], ret.at[rows(d), :], e_send.at[d - 1], e_recv.at[d - 1], dev(dp, lax.rem(me + d, E), p))

    def tc(d):
        return rc(tsrc, tland.at[d], t_send.at[d - 1], t_recv.at[d - 1], dev(dp, lax.rem(me + d, E), p))

    def go(d):
        ec(d).start()
        tc(d).start()

    each(go)
    ret_ref[pl.ds(0, cap), :] = sc[pl.ds(0, cap), :]
    tot_ref[0] = tsrc[...]
    drain(0)
    drain(1)
    each(lambda d: wc(d).wait_send())
    for k in range(1, N):
        rsc(k).wait_send()
        agc(k).wait_send()

    def fin(d):
        ec(d).wait()
        tc(d).wait()

    each(fin)
    rest = pl.ds(cap, R - cap)
    ret_ref[rest, :] = ret[rest, :]
    for d in range(1, E):
        tot_ref[d] = tland[d]


def body(
    inputs,
    cotangents,
    routes,
    gates,
    w_gate,
    w_up,
    w_down,
    proj_in,
    proj_out,
    proj_hid_a,
    proj_hid_b,
    queries,
):
    E = lax.axis_size("expert")
    DP = lax.axis_size("dp")
    NP = lax.axis_size("pipe")
    N = DP * NP
    count, width = inputs.shape
    cap = 4 * count // E
    nq = queries.shape[0]
    ff = w_gate.shape[2]
    ka = proj_in.shape[1]
    kb = proj_out.shape[1]
    L = 2 if DP % 2 == 0 else 1
    H = DP // L
    R = E * cap
    rk = R * ka // 128
    dense = cap >= count
    if dense:
        cap = count
        R = E * cap
        rk = R * ka // 128
        labels = jnp.arange(E, dtype=jnp.int32)
        hit = routes[None, :, :] == labels[:, None, None]
        slot_weight = jnp.sum(jnp.where(hit, gates[None, :, :], 0.0), axis=2)
        buf_in, buf_back = inputs[None], cotangents[None]
        picks = None
    else:
        picks, slot_weight = slot_matrix(routes, gates, E, cap)
        pick_rows = picks.astype(BF16)
        buf_in, buf_back = (
            jnp.dot(pick_rows, v, preferred_element_type=F32).astype(BF16).reshape(E, cap, width)
            for v in (inputs, cotangents)
        )
    weight_own = jnp.broadcast_to(slot_weight.reshape(E, cap, 1), (E, cap, nq))
    dims = (E, DP, NP, L, cap, ka, kb)
    V = pl.BlockSpec(memory_space=pltpu.VMEM)
    A = pl.BlockSpec(memory_space=pl.ANY)
    D = pltpu.SemaphoreType.DMA
    E1 = E - 1
    h1, p1 = max(H - 1, 1), max(NP - 1, 1)
    pairs = []
    for shape in (
        (2, E1),
        (2, h1, E1),
        (2, p1, E1),
        (2, h1, p1, E1),
        (2, h1, p1, E1),
        (2, H, NP, E1),
        (E1,),
        (N - 1,),
        (N - 1,),
        (E1,),
        (E1,),
    ):
        pairs += [D(shape), D(shape)]
    ret, tot = pl.pallas_call(
        functools.partial(mega, dims),
        name="routed_scores",
        out_shape=(
            jax.ShapeDtypeStruct((R, nq), F32),
            jax.ShapeDtypeStruct((E, 8, nq), F32),
        ),
        in_specs=[A, A, A, A, A, A, V, V, V, V, V],
        out_specs=(V, V),
        scratch_shapes=[
            pltpu.VMEM((R, width), BF16),
            pltpu.VMEM((R, width), BF16),
            pltpu.VMEM((width, ff), BF16),
            pltpu.VMEM((width, ff), BF16),
            pltpu.VMEM((ff, width), BF16),
            pltpu.VMEM((R, ff), F32),
            pltpu.VMEM((R, ff), F32),
            pltpu.VMEM((R, ka), F32),
            pltpu.VMEM((R, 2 * kb), F32),
            pltpu.VMEM((R + rk, 128), F32),
            pltpu.VMEM((N - 1, (R + rk) // N, 128), F32),
            pltpu.VMEM((R + rk, 128), F32),
            pltpu.VMEM((R, nq), F32),
            pltpu.VMEM((R, nq), F32),
            pltpu.VMEM((R, nq), F32),
            pltpu.VMEM((8, nq), F32),
            pltpu.VMEM((E, 8, nq), F32),
            D((6,)),
        ]
        + pairs,
        compiler_params=pltpu.CompilerParams(
            collective_id=0, has_side_effects=True, vmem_limit_bytes=62 * 1024 * 1024
        ),
    )(
        buf_in,
        buf_back,
        weight_own,
        w_gate,
        w_up,
        w_down,
        proj_in,
        jnp.concatenate([proj_out] * 2, axis=1),
        jnp.concatenate([proj_hid_a] * (128 // ka), axis=1),
        jnp.concatenate([proj_hid_b] * 2, axis=1),
        queries,
    )
    blocks = ret.reshape(E, cap, nq)
    if dense:
        token_scores = jnp.sum(blocks, axis=0)
    else:
        order = (lax.axis_index("expert") - jnp.arange(E) + E) % E
        token_scores = lax.dot_general(
            picks,
            blocks[order].reshape(R, nq),
            (((0,), (0,)), ((), ())),
            precision=lax.Precision.HIGHEST,
            preferred_element_type=F32,
        )
    scale = 1.0 / math.sqrt(count * E)
    return (token_scores, jnp.sum(tot[:, 0, :], axis=0) * scale)


def solution(mesh):
    both = ("dp", "pipe")
    placed = (
        P("expert", None),
        P("expert", None),
        P("expert", None),
        P("expert", None),
        P("expert", None, both),
        P("expert", None, both),
        P("expert", both, None),
        P(),
        P(),
        P(both, None),
        P(both, None),
        P(both, None),
    )
    return jax.shard_map(
        body,
        mesh=mesh,
        in_specs=placed,
        out_specs=(P("expert", both), P(both)),
        check_vma=False,
    )
```

```python
import functools
import math

import jax
import jax.numpy as jnp
from jax import lax
from jax.experimental import pallas as pl
from jax.experimental.pallas import tpu as pltpu
from jax.sharding import PartitionSpec as P

MESH = pl.DeviceIdType.MESH
F32 = jnp.float32
BF16 = jnp.bfloat16
NT = (((1,), (1,)), ((), ()))


def slot_matrix(route_rows, gate_rows, experts, capacity):
    count = route_rows.shape[0]
    flat = route_rows.reshape(-1)
    labels = jnp.arange(experts, dtype=jnp.int32)
    onehot = (flat[:, None] == labels[None, :]).astype(jnp.int32)
    earlier = jnp.cumsum(onehot, axis=0) - onehot
    position = jnp.sum(onehot * (labels[None, :] * capacity + earlier), axis=1)
    slot_ids = jnp.arange(experts * capacity, dtype=jnp.int32)
    table = (
        (position[None, :] == slot_ids[:, None]).astype(F32).reshape(experts * capacity, count, 2)
    )
    picks = jnp.sum(table, axis=2)
    weighted = jnp.sum(table * gate_rows[None, :, :], axis=(1, 2))
    return (picks, weighted)


def mega(
    dims,
    buf_in,
    buf_back,
    weight_own,
    wg_hbm,
    wu_hbm,
    wd_hbm,
    p_in,
    p_out,
    p_a,
    p_b,
    query,
    ret_ref,
    tot_ref,
    x_in,
    x_back,
    wg,
    wu,
    wd,
    gate_s,
    up_s,
    ain_s,
    bout_s,
    part,
    land,
    red,
    wl,
    sc,
    ret,
    tsrc,
    tland,
    local_sem,
    z_send,
    z_recv,
    y_send,
    y_recv,
    x_send,
    x_recv,
    g1_send,
    g1_recv,
    g2_send,
    g2_recv,
    c_send,
    c_recv,
    w_send,
    w_recv,
    rs_send,
    rs_recv,
    ag_send,
    ag_recv,
    e_send,
    e_recv,
    t_send,
    t_recv,
):
    E, DP, NP, L, cap, ka, kb = dims
    H = DP // L
    N = DP * NP
    R = E * cap
    width = x_in.shape[1]
    cw = width // N
    hw = cw // 2
    G = 128 // ka
    rk = R // G
    dp = lax.axis_index("dp")
    me = lax.axis_index("expert")
    p = lax.axis_index("pipe")
    h = dp // L
    l = dp % L
    s = dp * NP + p

    def dev(d, e, q):
        return {"dp": d, "expert": e, "pipe": q}

    locals_ = []
    dense = buf_in.shape[0] == 1
    own = 0 if dense else me
    for i, (src, dst) in enumerate(
        (
            (buf_in.at[own], x_in.at[pl.ds(0, cap), :]),
            (buf_back.at[own], x_back.at[pl.ds(0, cap), :]),
            (weight_own.at[me], wl.at[pl.ds(0, cap), :]),
            (wg_hbm.at[0], wg),
            (wu_hbm.at[0], wu),
            (wd_hbm.at[0], wd),
        )
    ):
        c = pltpu.make_async_copy(src, dst, local_sem.at[i])
        locals_.append(c)

    barrier = pltpu.get_barrier_semaphore()

    def plane(k):
        t = lax.rem(s + k, N)
        return dev(t // NP, me, t % NP)

    for k in range(1, N):
        pl.semaphore_signal(barrier, inc=1, device_id=plane(k), device_id_type=MESH)
    for k in range(1, E):
        pl.semaphore_signal(
            barrier, inc=1, device_id=dev(dp, lax.rem(me + k, E), p), device_id_type=MESH
        )
    pl.semaphore_wait(barrier, N + E - 2)

    bufs = (buf_in, buf_back)
    xs = (x_in, x_back)

    def rc(src, dst, ss, rs, to):
        return pltpu.make_async_remote_copy(
            src_ref=src, dst_ref=dst, send_sem=ss, recv_sem=rs, device_id=to, device_id_type=MESH
        )

    def cols(share, off=0, size=None):
        size = cw if size is None else size
        return pl.ds(pl.multiple_of(share * cw + off, 128), size)

    def rows(d):
        return pl.ds(pl.multiple_of(d * cap, 8), cap)

    def share(k, kp, lane=None):
        lane = l if lane is None else lane
        return (lax.rem(h - k + H, H) * L + lane) * NP + lax.rem(p - kp + NP, NP)

    def zc(a, d):
        dst = lax.rem(me - d + E, E)
        src = bufs[a].at[0 if dense else dst, :, cols(s)]
        return rc(src, xs[a].at[rows(d), cols(s)], z_send.at[a, d - 1], z_recv.at[a, d - 1], dev(dp, dst, p))

    def yc(a, k, d):
        r = xs[a].at[rows(d), cols(s)]
        return rc(r, r, y_send.at[a, k - 1, d - 1], y_recv.at[a, k - 1, d - 1], dev(lax.rem(h + k, H) * L + l, me, p))

    def xc(a, kp, d):
        r = xs[a].at[rows(d), cols(s)]
        return rc(r, r, x_send.at[a, kp - 1, d - 1], x_recv.at[a, kp - 1, d - 1], dev(dp, me, lax.rem(p + kp, NP)))

    def g1(a, k, kp, d):
        r = xs[a].at[rows(d), cols(share(k, 0), 0, hw)]
        i = (a, k - 1, kp - 1, d - 1)
        return rc(r, r, g1_send.at[i], g1_recv.at[i], dev(dp, me, lax.rem(p + kp, NP)))

    def g2(a, k, kp, d):
        r = xs[a].at[rows(d), cols(share(0, kp), hw, hw)]
        i = (a, k - 1, kp - 1, d - 1)
        return rc(r, r, g2_send.at[i], g2_recv.at[i], dev(lax.rem(h + k, H) * L + l, me, p))

    def cc(a, k, kp, d):
        r = xs[a].at[rows(d), cols(share(k, kp))]
        i = (a, k, kp, d - 1)
        return rc(r, r, c_send.at[i], c_recv.at[i], dev(h * L + (1 - l), me, p))

    def wc(d):
        dst = lax.rem(me - d + E, E)
        return rc(weight_own.at[dst], wl.at[rows(d), :], w_send.at[d - 1], w_recv.at[d - 1], dev(dp, dst, p))

    def each(fn):
        def step(i, carry):
            fn(i + 1)
            return carry

        lax.fori_loop(0, E - 1, step, 0)

    KS = range(1, H)
    PS = range(1, NP)

    def stage_a(a):
        def f(d):
            zc(a, d).wait_recv()
            for k in KS:
                yc(a, k, d).start()
            for kp in PS:
                xc(a, kp, d).start()
            if L > 1:
                cc(a, 0, 0, d).start()

        each(f)

    def stage_b(a):
        def f(d):
            for k in KS:
                yc(a, k, d).wait_recv()
                for kp in PS:
                    g1(a, k, kp, d).start()
                if L > 1:
                    cc(a, k, 0, d).start()
            for kp in PS:
                xc(a, kp, d).wait_recv()
                for k in KS:
                    g2(a, k, kp, d).start()
                if L > 1:
                    cc(a, 0, kp, d).start()

        each(f)

    def stage_c(a):
        def f(d):
            for k in KS:
                for kp in PS:
                    g1(a, k, kp, d).wait_recv()
                    g2(a, k, kp, d).wait_recv()
                    if L > 1:
                        cc(a, k, kp, d).start()

        each(f)

    def stage_d(a):
        def f(d):
            if L > 1:
                for k in range(H):
                    for kp in range(NP):
                        cc(a, k, kp, d).wait_recv()

        each(f)

    def drain(a):
        def f(d):
            zc(a, d).wait_send()
            for k in KS:
                yc(a, k, d).wait_send()
            for kp in PS:
                xc(a, kp, d).wait_send()
            for k in KS:
                for kp in PS:
                    g1(a, k, kp, d).wait_send()
                    g2(a, k, kp, d).wait_send()
            if L > 1:
                for k in range(H):
                    for kp in range(NP):
                        cc(a, k, kp, d).wait_send()

        each(f)

    each(lambda d: zc(0, d).start())
    each(lambda d: zc(1, d).start())
    for c in locals_:
        c.start()
    each(lambda d: wc(d).start())
    stage_a(0)
    stage_b(0)
    stage_a(1)
    stage_c(0)
    stage_d(0)
    for i in (0, 3, 4):
        locals_[i].wait()

    MT = min(256, R)
    T = R // MT
    lane = lax.broadcasted_iota(jnp.int32, (MT, 128), 1)
    part[pl.ds(R, rk), :] = jnp.zeros((rk, 128), F32)

    def wide(v, proj, times):
        return lax.dot_general(
            v, jnp.concatenate([proj[...]] * times, axis=0), NT, preferred_element_type=F32
        )

    def gate_up(m):
        rr = pl.ds(pl.multiple_of(m * MT, MT), MT)
        x = x_in[rr, :]
        g = jnp.dot(x, wg[...], preferred_element_type=F32)
        gate_s[rr, :] = g
        u = jnp.dot(x, wu[...], preferred_element_type=F32)
        up_s[rr, :] = u
        ain_s[rr, :] = lax.dot_general(x, p_in[...], NT, preferred_element_type=F32)

    def factor_a(m):
        rr = pl.ds(pl.multiple_of(m * MT, MT), MT)
        g = gate_s[rr, :]
        u = up_s[rr, :]
        sg = jax.nn.sigmoid(g)
        gs = g * sg
        hid = (gs * u).astype(BF16)
        gate_s[rr, :] = gs
        up_s[rr, :] = u * sg * (1.0 + g * (1.0 - sg))
        at = wide(hid, p_a, 128 // ka)
        for j in range(MT // rk):
            grp = m * (MT // rk) + j
            piece = at[j * rk : (j + 1) * rk, :]
            part[pl.ds(R, rk), :] += jnp.where(lane[:rk] // ka == grp, piece, 0.0)

    def down(m):
        rr = pl.ds(pl.multiple_of(m * MT, MT), MT)
        x = x_back[rr, :]
        back = lax.dot_general(x, wd[...], NT, preferred_element_type=F32)
        bout_s[rr, :] = wide(x, p_out, 2)
        du = (back * gate_s[rr, :]).astype(BF16)
        dg = (back * up_s[rr, :]).astype(BF16)
        bu = wide(du, p_b, 2)
        bg = wide(dg, p_b, 2)
        part[rr, :] = jnp.where(lane < kb, bu, bg)

    half = (T + 1) // 2
    pl.loop(0, half)(gate_up)
    stage_b(1)
    if T > half:
        pl.loop(half, T)(gate_up)
    stage_c(1)
    pl.loop(0, T)(factor_a)
    stage_d(1)
    locals_[1].wait()
    locals_[5].wait()
    pl.loop(0, T)(down)

    ch = (R + rk) // N

    def chunk(i):
        return pl.ds(pl.multiple_of(i * ch, 8), ch)

    def rsc(k):
        t = lax.rem(s + k, N)
        return rc(part.at[chunk(t), :], land.at[k - 1], rs_send.at[k - 1], rs_recv.at[k - 1], plane(k))

    def agc(k):
        r = red.at[chunk(s), :]
        return rc(r, r, ag_send.at[k - 1], ag_recv.at[k - 1], plane(k))

    for k in range(1, N):
        rsc(k).start()
    for k in range(1, N):
        rsc(k).wait_recv()
    total = part[chunk(s), :]
    for k in range(1, N):
        total = total + land[k - 1]
    red[chunk(s), :] = total
    for k in range(1, N):
        agc(k).start()
    each(lambda d: wc(d).wait_recv())
    locals_[2].wait()
    for k in range(1, N):
        t = lax.rem(s - k + N, N)
        r = red.at[chunk(t), :]
        rc(r, r, ag_send.at[k - 1], ag_recv.at[k - 1], plane(k)).wait_recv()

    seg = ka * kb
    lane_k = lax.broadcasted_iota(jnp.int32, (rk, 128), 1)

    def split(a):
        hi = a.astype(BF16)
        return hi, (a - hi.astype(F32)).astype(BF16)

    def spread(a, first):
        depth = a.shape[1]
        row = lax.broadcasted_iota(jnp.int32, (depth, seg), 0)
        col = lax.broadcasted_iota(jnp.int32, (depth, seg), 1)
        sel = jnp.where(row - first == col // kb, 1.0, 0.0).astype(BF16)
        hi, lo = split(a)
        return jnp.dot(hi, sel, preferred_element_type=F32) + jnp.dot(
            lo, sel, preferred_element_type=F32
        )

    def score(k):
        rr = pl.ds(pl.multiple_of(k * rk, 8), rk)
        b = red[rr, :]
        br = pltpu.roll(b, kb, 1)
        bu = jnp.where(lane_k < kb, b, br)
        bg = jnp.where(lane_k < kb, br, b)
        ah = spread(red[pl.ds(R, rk), :], k * ka)
        ai = spread(ain_s[rr, :], 0)
        q = query[...]
        reps = seg // 128

        def seg_dot(a, bb, i):
            sk = jnp.concatenate(
                [(a[:, j * 128 : (j + 1) * 128] * bb).astype(BF16) for j in range(reps)], axis=1
            )
            return lax.dot_general(
                sk, q[:, i * seg : (i + 1) * seg], NT, preferred_element_type=F32
            )

        r = seg_dot(ah, bout_s[rr, :], 0) + seg_dot(ai, bu, 1) + seg_dot(ai, bg, 2)
        sc[rr, :] = r * wl[rr, :]

    pl.loop(0, G)(score)
    tsrc[...] = jnp.broadcast_to(jnp.sum(sc[...], axis=0, keepdims=True), tsrc.shape)

    def ec(d):
        return rc(sc.at[rows(d), :], ret.at[rows(d), :], e_send.at[d - 1], e_recv.at[d - 1], dev(dp, lax.rem(me + d, E), p))

    def tc(d):
        return rc(tsrc, tland.at[d], t_send.at[d - 1], t_recv.at[d - 1], dev(dp, lax.rem(me + d, E), p))

    def go(d):
        ec(d).start()
        tc(d).start()

    each(go)
    ret_ref[pl.ds(0, cap), :] = sc[pl.ds(0, cap), :]
    tot_ref[0] = tsrc[...]
    drain(0)
    drain(1)
    each(lambda d: wc(d).wait_send())
    for k in range(1, N):
        rsc(k).wait_send()
        agc(k).wait_send()

    def fin(d):
        ec(d).wait()
        tc(d).wait()

    each(fin)
    rest = pl.ds(cap, R - cap)
    ret_ref[rest, :] = ret[rest, :]
    for d in range(1, E):
        tot_ref[d] = tland[d]


def body(
    inputs,
    cotangents,
    routes,
    gates,
    w_gate,
    w_up,
    w_down,
    proj_in,
    proj_out,
    proj_hid_a,
    proj_hid_b,
    queries,
):
    E = lax.axis_size("expert")
    DP = lax.axis_size("dp")
    NP = lax.axis_size("pipe")
    N = DP * NP
    count, width = inputs.shape
    cap = 4 * count // E
    nq = queries.shape[0]
    ff = w_gate.shape[2]
    ka = proj_in.shape[1]
    kb = proj_out.shape[1]
    L = 2 if DP % 2 == 0 else 1
    H = DP // L
    R = E * cap
    rk = R * ka // 128
    dense = cap >= count
    if dense:
        cap = count
        R = E * cap
        rk = R * ka // 128
        labels = jnp.arange(E, dtype=jnp.int32)
        hit = routes[None, :, :] == labels[:, None, None]
        slot_weight = jnp.sum(jnp.where(hit, gates[None, :, :], 0.0), axis=2)
        buf_in, buf_back = inputs[None], cotangents[None]
        picks = None
    else:
        picks, slot_weight = slot_matrix(routes, gates, E, cap)
        pick_rows = picks.astype(BF16)
        buf_in, buf_back = (
            jnp.dot(pick_rows, v, preferred_element_type=F32).astype(BF16).reshape(E, cap, width)
            for v in (inputs, cotangents)
        )
    weight_own = jnp.broadcast_to(slot_weight.reshape(E, cap, 1), (E, cap, nq))
    dims = (E, DP, NP, L, cap, ka, kb)
    V = pl.BlockSpec(memory_space=pltpu.VMEM)
    A = pl.BlockSpec(memory_space=pl.ANY)
    D = pltpu.SemaphoreType.DMA
    E1 = E - 1
    h1, p1 = max(H - 1, 1), max(NP - 1, 1)
    pairs = []
    for shape in (
        (2, E1),
        (2, h1, E1),
        (2, p1, E1),
        (2, h1, p1, E1),
        (2, h1, p1, E1),
        (2, H, NP, E1),
        (E1,),
        (N - 1,),
        (N - 1,),
        (E1,),
        (E1,),
    ):
        pairs += [D(shape), D(shape)]
    ret, tot = pl.pallas_call(
        functools.partial(mega, dims),
        name="routed_scores",
        out_shape=(
            jax.ShapeDtypeStruct((R, nq), F32),
            jax.ShapeDtypeStruct((E, 8, nq), F32),
        ),
        in_specs=[A, A, A, A, A, A, V, V, V, V, V],
        out_specs=(V, V),
        scratch_shapes=[
            pltpu.VMEM((R, width), BF16),
            pltpu.VMEM((R, width), BF16),
            pltpu.VMEM((width, ff), BF16),
            pltpu.VMEM((width, ff), BF16),
            pltpu.VMEM((ff, width), BF16),
            pltpu.VMEM((R, ff), F32),
            pltpu.VMEM((R, ff), F32),
            pltpu.VMEM((R, ka), F32),
            pltpu.VMEM((R, 2 * kb), F32),
            pltpu.VMEM((R + rk, 128), F32),
            pltpu.VMEM((N - 1, (R + rk) // N, 128), F32),
            pltpu.VMEM((R + rk, 128), F32),
            pltpu.VMEM((R, nq), F32),
            pltpu.VMEM((R, nq), F32),
            pltpu.VMEM((R, nq), F32),
            pltpu.VMEM((8, nq), F32),
            pltpu.VMEM((E, 8, nq), F32),
            D((6,)),
        ]
        + pairs,
        compiler_params=pltpu.CompilerParams(
            collective_id=0, has_side_effects=True, vmem_limit_bytes=62 * 1024 * 1024
        ),
    )(
        buf_in,
        buf_back,
        weight_own,
        w_gate,
        w_up,
        w_down,
        proj_in.T,
        proj_out.T,
        proj_hid_a.T,
        proj_hid_b.T,
        queries,
    )
    blocks = ret.reshape(E, cap, nq)
    if dense:
        token_scores = jnp.sum(blocks, axis=0)
    else:
        order = (lax.axis_index("expert") - jnp.arange(E) + E) % E
        token_scores = lax.dot_general(
            picks,
            blocks[order].reshape(R, nq),
            (((0,), (0,)), ((), ())),
            precision=lax.Precision.HIGHEST,
            preferred_element_type=F32,
        )
    scale = 1.0 / math.sqrt(count * E)
    return (token_scores, jnp.sum(tot[:, 0, :], axis=0) * scale)


def solution(mesh):
    both = ("dp", "pipe")
    placed = (
        P("expert", None),
        P("expert", None),
        P("expert", None),
        P("expert", None),
        P("expert", None, both),
        P("expert", None, both),
        P("expert", both, None),
        P(),
        P(),
        P(both, None),
        P(both, None),
        P(both, None),
    )
    return jax.shard_map(
        body,
        mesh=mesh,
        in_specs=placed,
        out_specs=(P("expert", both), P(both)),
        check_vma=False,
    )
```
